256 devices in a mesh: mp: 2 (over z_hi), dp: 128 (over z_lo, y, x, core).
Axes of the slice: x: 4, y: 4, z: 8 (z_hi: 2, z_lo: 4; z = z_hi * 4 + z_lo), core: 2. Of those that a mesh axis runs over, the one named last changes fastest.
Arguments:
- image: bfloat16 [128, 128, 1024], P('dp', 'mp'), may hold values from -8 to 8
- text: bfloat16 [16384, 1024], P('dp'), may hold values from -8 to 8
- logit_scale: float32 [1], replicated, may hold values from 10 to 30
Outputs:
- row_loss: float32 [128, 128], P('dp', 'mp')
- col_loss: float32 [128, 128], P('dp', 'mp')
The draws below stay inside these ranges and needn't reach their ends.
All inputs are finite; a program needn't handle non-finite values.
Results may differ from the reference program's by a relative error of at most 0.012.
Values may be sent and summed in bfloat16 or wider, within the bound.
No kernel may reach another device: no remote copies, remote signals or barrier semaphores. Data moves between devices by JAX's collectives and lax.ppermute only.
A program may use at most 128 MiB of HBM per device.

```python
import math
import jax
import jax.numpy as jnp
from jax import lax

D = 1024
TOK_DEV = 128
TOKENS = 16384
N_DP = 128


def pair_rows(key):
    folded = jax.random.fold_in(key, 4099)
    subkeys = jax.random.split(folded, 7)
    groups = TOKENS // 8
    centers = jax.random.normal(subkeys[0], (groups, D), jnp.float32)
    members = jax.random.randint(subkeys[1], (TOKENS,), 0, groups)
    center_rows = centers[members]
    picture_pull = jax.random.uniform(subkeys[2], (TOKENS, 1), jnp.float32, minval=0.0, maxval=0.95)
    caption_pull = jax.random.uniform(subkeys[3], (TOKENS, 1), jnp.float32, minval=0.3, maxval=0.95)
    matching = jax.random.uniform(subkeys[4], (TOKENS, 1), jnp.float32, minval=0.0, maxval=0.7)
    picture_noise = jax.random.normal(subkeys[5], (TOKENS, D), jnp.float32)
    caption_noise = jax.random.normal(subkeys[6], (TOKENS, D), jnp.float32)
    picture = picture_pull * center_rows + jnp.sqrt(1.0 - picture_pull * picture_pull) * picture_noise
    caption_side = caption_pull * center_rows + jnp.sqrt(1.0 - caption_pull * caption_pull) * caption_noise
    caption = matching * picture + jnp.sqrt(1.0 - matching * matching) * caption_side
    return (jnp.clip(picture, -8.0, 8.0), jnp.clip(caption, -8.0, 8.0))


def draw_image(key, part):
    picture = pair_rows(key)[0]
    return picture.reshape(N_DP, TOK_DEV, D).astype(jnp.bfloat16)


def draw_text(key, part):
    caption = pair_rows(key)[1]
    return caption.astype(jnp.bfloat16)


def setup_inputs(seed: int = 0) -> dict:
    arg_keys = jax.random.split(jax.random.key(seed), 4)
    image = draw_image(jax.random.fold_in(arg_keys[3], 71), 0)
    text = draw_text(jax.random.fold_in(arg_keys[3], 71), 0)
    logit_scale = jnp.clip(jnp.exp(jax.random.uniform(arg_keys[2], (1,), jnp.float32, math.log(10.0), math.log(30.0))), 10.0, 30.0)
    return {"image": image, "text": text, "logit_scale": logit_scale}


def normalize(rows):
    wide = rows.astype(jnp.float32)
    return (wide * lax.rsqrt(lax.optimization_barrier(jnp.sum(wide * wide, axis=1, keepdims=True)) + 1e-06)).astype(jnp.bfloat16)

def reference(image, text, logit_scale):
    scale = logit_scale[0]
    img_n = normalize(image.reshape(TOKENS, D))
    text_n = normalize(text)
    diag = scale * lax.optimization_barrier(jnp.sum(img_n.astype(jnp.float32) * text_n.astype(jnp.float32), axis=1))
    block = TOK_DEV * 4
    blocks = img_n.reshape(TOKENS // block, block, D)

    def step(col_total, rows):
        scores = scale * jnp.dot(rows, text_n.T, preferred_element_type=jnp.float32)
        weights = jnp.exp(scores)
        return (col_total + lax.optimization_barrier(jnp.sum(weights, axis=0)), lax.optimization_barrier(jnp.sum(weights, axis=1)))
    col_total, row_total = lax.scan(step, jnp.zeros((TOKENS,), jnp.float32), blocks)
    row_total = row_total.reshape(TOKENS)
    row_loss = (jnp.log(row_total) - diag).reshape(N_DP, TOK_DEV)
    col_loss = (jnp.log(col_total) - diag).reshape(N_DP, TOK_DEV)
    return (row_loss, col_loss)
```

```python
import jax
import jax.numpy as jnp
import numpy as np
from jax import lax
from jax.sharding import Mesh, PartitionSpec as P

AXES = ("h", "l", "y", "x", "c")
SIZES = (2, 4, 4, 4, 2)


def moved(place, x=0, y=0, z=0, c=0):
    h, low, py, px, pc = place
    pz = (h * 4 + low + z) % 8
    return (pz // 4, pz % 4, (py + y) % 4, (px + x) % 4, (pc + c) % 2)


def permute(array, target):
    pairs = []
    for place in np.ndindex(SIZES):
        goal = target(place)
        if goal is not None:
            pairs.append(
                (int(np.ravel_multi_index(place, SIZES)), int(np.ravel_multi_index(goal, SIZES)))
            )
    return lax.ppermute(array, AXES, pairs)


def by_core(array, zero, one):
    return permute(array, lambda place: moved(place, **(one if place[4] else zero)))


def swap_cores(array):
    return permute(array, lambda place: moved(place, c=1))


def ring_partner(position, length, turn):
    if turn == 2:
        return {0: 3, 3: 0, 1: 6, 6: 1, 2: 5, 5: 2, 4: 7, 7: 4}[position]
    if turn == 0:
        return position ^ 1
    return (position + (1 if position % 2 else -1)) % length


def reduce_round(turn):
    def target(place):
        h, low, y, x, c = place
        if c == 0:
            if turn < 2:
                return (h, low, y, ring_partner(x, 4, turn), c)
            return (h, low, ring_partner(y, 4, turn - 2), x, c)
        if turn == 3:
            return None
        z = ring_partner(h * 4 + low, 8, turn)
        return (z // 4, z % 4, y, x, c)

    return target


def normalize(rows):
    wide = rows.astype(jnp.float32)
    return (wide * lax.rsqrt(jnp.sum(wide * wide, axis=1, keepdims=True) + 1e-06)).astype(
        jnp.bfloat16
    )


def rolled(array, shift, axis):
    array = jnp.where(shift % 2 == 1, jnp.roll(array, 1, axis), array)
    return jnp.where(shift // 2 == 1, jnp.roll(array, 2, axis), array)


def on_device(image, text, logit_scale):
    scale = logit_scale[0]
    own_img = normalize(image[0])
    half = own_img.shape[0]
    text_n = normalize(text)
    h, low, y, x, c = (lax.axis_index(a) for a in AXES)
    first = c == 0
    own_text = lax.dynamic_slice_in_dim(text_n, h * half, half, 0)
    diag = scale * jnp.sum(own_img.astype(jnp.float32) * own_text.astype(jnp.float32), axis=1)

    other_text = swap_cores(text_n)
    chip_text = jnp.where(
        first,
        jnp.concatenate([text_n, other_text], axis=0),
        jnp.concatenate([other_text, text_n], axis=0),
    )
    below = by_core(own_img, dict(x=1), dict(y=1))
    above = by_core(own_img, dict(x=-1), dict(y=-1))
    text_a = by_core(chip_text, dict(z=1), dict(z=-1))
    far_a = by_core(below[: half // 2], dict(x=1), dict(y=1))
    far_b = by_core(above[half // 2 :], dict(x=-1), dict(y=-1))
    line = jnp.concatenate([own_img, below, above, far_a, far_b], axis=0)
    line_below = by_core(line, dict(y=1), dict(x=1))
    line_above = by_core(line, dict(y=-1), dict(x=-1))
    text_b = swap_cores(text_a)
    count = text_a.shape[0] // 2
    text_d = by_core(
        jnp.where(first, text_a[:count], text_a[count:]), dict(z=1), dict(z=-1)
    )
    text_e = swap_cores(text_d)
    span = line.shape[0] // 2
    line_far_a = by_core(line_below[:span], dict(y=1), dict(x=1))
    line_far_b = by_core(line_above[span:], dict(y=-1), dict(x=-1))

    rows = jnp.concatenate([line, line_below, line_above, line_far_a, line_far_b], axis=0)
    cols = jnp.concatenate([chip_text, text_a, text_b, text_d, text_e], axis=0)
    scores = scale * jnp.einsum("hd,cd->hc", rows, cols, preferred_element_type=jnp.float32)
    weights = jnp.exp(scores)
    row_part = jnp.sum(weights, axis=1)
    col_part = jnp.sum(weights, axis=0)

    row_part = row_part.reshape(4, 4, half)
    row_part = jnp.stack([row_part[k] for k in (0, 2, 3, 1)], axis=0)
    row_part = jnp.stack([row_part[:, k] for k in (0, 2, 3, 1)], axis=1)
    row_part = rolled(row_part, jnp.where(first, y, x), 0)
    row_part = rolled(row_part, jnp.where(first, x, y), 1)
    row_part = jnp.where(first, row_part, row_part.transpose(1, 0, 2)).reshape(-1)

    width = chip_text.shape[0]
    own, part_a, part_b, part_d, part_e = jnp.split(
        col_part, [width, 2 * width, 3 * width, 3 * width + count]
    )
    col_rel = jnp.stack(
        [
            own,
            jnp.where(first, part_b, part_a),
            jnp.where(
                first, jnp.concatenate([part_d, part_e]), jnp.concatenate([part_e, part_d])
            ),
            jnp.where(first, part_a, part_b),
        ]
    )
    col_part = rolled(col_rel, low, 0).reshape(-1)

    got = swap_cores(jnp.where(first, col_part, row_part))
    buffer = jnp.where(
        first,
        jnp.concatenate([row_part, got]),
        jnp.concatenate([col_part + got, jnp.zeros_like(got)]),
    )
    for turn in range(4):
        buffer = buffer + permute(buffer, reduce_round(turn))
    row_pair = lax.dynamic_slice_in_dim(
        buffer.reshape(2, 16, half), y * 4 + x, 1, 1
    ).reshape(2, half)
    col_pair = lax.dynamic_slice_in_dim(
        lax.dynamic_slice_in_dim(buffer[: 4 * width].reshape(4, 2, 2, half), low, 1, 0),
        h, 1, 2,
    ).reshape(2, half)
    back = swap_cores(jnp.where(first, row_pair[1], col_pair[0]))
    row_total = jnp.where(first, row_pair[0], back)
    col_total = jnp.where(first, back, col_pair[1])
    row_loss = (jnp.log(row_total) - diag).reshape(1, half)
    col_loss = (jnp.log(col_total) - diag).reshape(1, half)
    return (row_loss, col_loss)


def solution(mesh):
    grid = Mesh(mesh.devices.reshape(SIZES), AXES)
    pairs = ("l", "y", "x", "c")
    return jax.shard_map(
        on_device,
        mesh=grid,
        in_specs=(P(pairs, "h", None), P(pairs, None), P()),
        out_specs=(P(pairs, "h"), P(pairs, "h")),
        check_vma=False,
    )
```
